256 devices in a mesh: frame: 32 (over y_hi, z, core), stream: 8 (over y_lo, x).
Axes of the slice: x: 4, y: 4 (y_hi: 2, y_lo: 2; y = y_hi * 2 + y_lo), z: 8, core: 2. Of those that a mesh axis runs over, the one named last changes fastest.
Arguments:
- query: bfloat16 [8, 4096, 4096], P('stream', 'frame'), may hold values from -60 to 60
- key: bfloat16 [8, 4096, 4096], P('stream', 'frame'), may hold values from -4 to 4
- value: bfloat16 [8, 4096, 4096], P('stream', 'frame'), may hold values from -24 to 24
- latent: bfloat16 [8, 4096, 4096], P('stream', 'frame'), may hold values from -6 to 6
- target: bfloat16 [8, 4096, 4096], P('stream', 'frame'), may hold values from -6 to 6
- noise_level: float32 [8, 16], P('stream'), may hold values from 0.02 to 0.98
- mod_weight: bfloat16 [4096, 256], replicated, may hold values from -0.375 to 0.375
- block_order: int32 [64], replicated, may hold values from 0 to 63, as said below
- context_start: int32 [8, 16], P('stream'), may hold values from 0 to 15, as said below
Outputs:
- grad_weight: float32 [4096, 256], P('frame')
The draws below stay inside these ranges and needn't reach their ends.
Inputs may be any that keep to these rules, and one draw needn't show every extreme that they name: block_order is a permutation of 0 to 63, and entries 2 i and 2 i + 1 add up to 63. context_start[s, c] lies between 0 and c.
All inputs are finite; a program needn't handle non-finite values.
Results may differ from the reference program's by a relative error of at most 0.0016.
Values may be sent and summed in bfloat16 or wider, within the bound.
No kernel may reach another device: no remote copies, remote signals or barrier semaphores. Data moves between devices by JAX's collectives and lax.ppermute only.
A program may use at most 64 MiB of HBM per device.

```python
import math
import jax
import jax.numpy as jnp
from jax import lax

HEAD_DIM = 128
HEADS = 32
D = 4096
FREQ = 256
GROUPS = 16
BLOCK_LEN = 64
BLOCKS = 64
SEQ = 4096
GROUP_LEN = 256
STREAMS = 8
N_FRAME = 32


def drawn_pair(key):
    shape = (STREAMS, SEQ, D)
    keys = jnp.clip(jax.random.normal(jax.random.fold_in(key, 101), shape, jnp.float32), -4.0, 4.0)
    queries = jnp.clip(jax.random.normal(jax.random.fold_in(key, 202), shape, jnp.float32), -4.0, 4.0)
    return (queries, keys)


def draw_query(key, part):
    pair = drawn_pair(key)
    return pair[0].astype(jnp.bfloat16)


def draw_key(key, part):
    pair = drawn_pair(key)
    return pair[1].astype(jnp.bfloat16)


def draw_block_order(key, part):
    order = jax.random.permutation(jax.random.fold_in(key, 11), N_FRAME).astype(jnp.int32)
    flipped = jax.random.randint(jax.random.fold_in(key, 12), (N_FRAME,), 0, 2)
    first = jnp.where(flipped == 1, BLOCKS - 1 - order, order)
    second = BLOCKS - 1 - first
    return jnp.stack([first, second], axis=1).reshape(BLOCKS).astype(jnp.int32)


def draw_context_start(key, part):
    upper = jnp.arange(GROUPS, dtype=jnp.int32)[None, :] + 1
    return jax.random.randint(jax.random.fold_in(key, 21), (STREAMS, GROUPS), 0, upper).astype(jnp.int32)


def steps_of(own_key, extent, split, low, top_value):
    level = 1.0
    for axis_at, shards_of in split:
        draws = jax.random.uniform(jax.random.fold_in(jax.random.fold_in(own_key, 6), axis_at), (shards_of,), jnp.float32, low / len(split), top_value / len(split))
        level = level * jnp.repeat(jnp.exp(draws), extent[axis_at] // shards_of).reshape((-1,) + (1,) * (len(extent) - 1 - axis_at))
    return level


def normal_values(rng, dims, spread, bound, split=(), kind=jnp.bfloat16):
    result = jax.random.normal(rng, dims, jnp.float32) * spread
    if len(split) > 0:
        result = steps_of(rng, dims, split, -0.22, 0.18) * result
    return jnp.clip(result, min=-bound, max=bound).astype(kind)


def setup_inputs(seed: int = 0) -> dict:
    streams_of = jax.random.split(jax.random.key(seed), 10)
    return {
        "query": draw_query(jax.random.fold_in(streams_of[9], 71), 0),
        "key": draw_key(jax.random.fold_in(streams_of[9], 71), 0),
        "value": normal_values(streams_of[2], (STREAMS, SEQ, D), 4.0, 24.0, ((0, 8), (1, 32))),
        "latent": normal_values(streams_of[3], (STREAMS, SEQ, D), 1.0, 6.0, ((0, 8), (1, 32))),
        "target": normal_values(streams_of[4], (STREAMS, SEQ, D), 1.0, 6.0, ((0, 8), (1, 32))),
        "noise_level": jnp.clip(0.02 + 0.96000002 * jax.random.uniform(streams_of[5], (STREAMS, GROUPS), jnp.float32) ** steps_of(streams_of[5], (STREAMS, GROUPS), ((0, 8),), -0.2, 0.2), 0.02, 0.98),
        "mod_weight": normal_values(streams_of[6], (D, FREQ), FREQ ** -0.5, 0.375),
        "block_order": draw_block_order(jax.random.fold_in(streams_of[9], 71), 0),
        "context_start": draw_context_start(jax.random.fold_in(streams_of[9], 71), 0),
    }


def reference(query, key, value, latent, target, noise_level, mod_weight, block_order, context_start):
    half_width = FREQ // 2
    frequency = jnp.exp(-math.log(10000.0) * jnp.arange(half_width, dtype=jnp.float32) / half_width)
    angles = 1000.0 * noise_level[..., None] * frequency
    embed = jnp.concatenate([jnp.cos(angles), jnp.sin(angles)], -1).astype(jnp.bfloat16)
    gate = jnp.dot(embed.reshape(STREAMS * GROUPS, FREQ), mod_weight.T, preferred_element_type=jnp.float32)
    gate = gate.reshape(STREAMS, GROUPS, D)
    block_group = (block_order // (BLOCKS // GROUPS)).astype(jnp.int32)
    row_group = block_group[jnp.arange(SEQ, dtype=jnp.int32) // BLOCK_LEN]
    scale = 1.0 / math.sqrt(HEAD_DIM)

    def one_stream(stream):
        row_start = context_start[stream][row_group]
        visible = (row_start[:, None] <= row_group[None, :]) & (row_group[None, :] <= row_group[:, None])
        queries = query[stream].reshape(SEQ, HEADS, HEAD_DIM).transpose(1, 0, 2)
        keys = key[stream].reshape(SEQ, HEADS, HEAD_DIM).transpose(1, 0, 2)
        values = value[stream].reshape(SEQ, HEADS, HEAD_DIM).transpose(1, 0, 2)

        def one_head(parts):
            scores = jnp.dot(parts[0], parts[1].T, preferred_element_type=jnp.float32) * scale
            masked = jnp.where(visible, scores, -jnp.inf)
            peak = lax.optimization_barrier(jnp.max(masked, axis=-1, keepdims=True))
            unnorm = jnp.where(visible, jnp.exp(masked - peak), 0.0)
            probs = (unnorm / lax.optimization_barrier(jnp.sum(unnorm, axis=-1, keepdims=True))).astype(jnp.bfloat16)
            return jnp.dot(probs, parts[2], preferred_element_type=jnp.float32).astype(jnp.bfloat16)
        heads_out = lax.map(one_head, (queries, keys, values))
        attn_wide = heads_out.transpose(1, 0, 2).reshape(SEQ, D).astype(jnp.float32)
        error = latent[stream].astype(jnp.float32) + gate[stream][row_group] * attn_wide - target[stream].astype(jnp.float32)
        return jax.ops.segment_sum(attn_wide * error, row_group, num_segments=GROUPS)
    group_sum = lax.map(one_stream, jnp.arange(STREAMS, dtype=jnp.int32))
    grad_weight = jnp.dot(group_sum.reshape(STREAMS * GROUPS, D).T, embed.astype(jnp.float32).reshape(STREAMS * GROUPS, FREQ), precision=lax.Precision.HIGHEST)
    return grad_weight / math.sqrt(GROUP_LEN)
```

```python
import functools
import math

import jax
import jax.numpy as jnp
from jax import lax
from jax.experimental import pallas as pl
from jax.experimental.pallas import tpu as pltpu
from jax.sharding import PartitionSpec as P

HEAD_DIM = 128
CHUNK = 4


def panels_kernel(*refs, panel):
    ins, out = refs[:-1], refs[-1]
    rows = ins[0].shape[0]
    for k in range(out.shape[0]):
        for a, ref in enumerate(ins):
            out[k, a * rows : (a + 1) * rows, :] = ref[:, k * panel : (k + 1) * panel]


def difference_kernel(latent, target, out, *, panel):
    for k in range(out.shape[0]):
        part = slice(k * panel, (k + 1) * panel)
        wide = latent[:, part].astype(jnp.float32) - target[:, part].astype(jnp.float32)
        out[k] = wide.astype(jnp.bfloat16)


def to_panels(kernel, arrays, frames, stacked):
    rows, width = arrays[0].shape
    panel = width // frames
    step = max(1, frames // 4)
    return pl.pallas_call(
        functools.partial(kernel, panel=panel),
        grid=(frames // step,),
        in_specs=[pl.BlockSpec((rows, step * panel), lambda i: (0, i))] * len(arrays),
        out_specs=pl.BlockSpec((step, stacked * rows, panel), lambda i: (i, 0, 0)),
        out_shape=jax.ShapeDtypeStruct((frames, stacked * rows, panel), jnp.bfloat16),
    )(*arrays)


def attend_kernel(
    place, start, qkv, gate, attn_out, square_out, q_sorted, k_sorted, v_sorted, strip, *, per_group, groups
):
    block_len, dim = qkv.shape[1], qkv.shape[2]
    blocks = per_group * groups
    rows = per_group * block_len
    scale = 1.0 / math.sqrt(dim)

    def sort_block(t, carry):
        p = place[t]
        base = (p // 2) * 6 + p % 2
        at = pl.ds(pl.multiple_of(t * block_len, block_len), block_len)
        q_sorted[at, :] = qkv[base]
        k_sorted[at, :] = qkv[base + 2]
        v_sorted[at, :] = qkv[base + 4]
        return carry

    lax.fori_loop(0, blocks, sort_block, 0, unroll=8)
    pad = jnp.zeros(((CHUNK - 1) * rows, dim), jnp.bfloat16)
    k_sorted[blocks * block_len :, :] = pad
    v_sorted[blocks * block_len :, :] = pad

    def one_group(c, carry):
        first = start[c]
        count = c - first + 1
        chunks = (count + CHUNK - 1) // CHUNK
        at_q = pl.ds(pl.multiple_of(c * rows, rows), rows)
        q = q_sorted[at_q, :]

        def scores(i, peak):
            for u in range(CHUNK):
                g = first + i * CHUNK + u
                k = k_sorted[pl.ds(pl.multiple_of(g * rows, rows), rows), :]
                s = lax.dot_general(
                    q, k, (((1,), (1,)), ((), ())), preferred_element_type=jnp.float32
                )
                s = jnp.where(g <= c, s * scale, -jnp.inf)
                strip[i * CHUNK + u] = s
                for b in range(rows // 128):
                    peak = jnp.maximum(peak, s[:, b * 128 : (b + 1) * 128])
            return peak

        peak = lax.fori_loop(0, chunks, scores, jnp.full((rows, 128), -jnp.inf, jnp.float32))
        peak = jnp.max(peak, axis=1, keepdims=True)

        def exponents(i, total):
            for u in range(CHUNK):
                e = jnp.exp(strip[i * CHUNK + u] - peak)
                strip[i * CHUNK + u] = e
                for b in range(rows // 128):
                    total = total + e[:, b * 128 : (b + 1) * 128]
            return total

        total = lax.fori_loop(0, chunks, exponents, jnp.zeros((rows, 128), jnp.float32))
        inverse = 1.0 / jnp.sum(total, axis=1, keepdims=True)

        def weigh(i, acc):
            for u in range(CHUNK):
                g = first + i * CHUNK + u
                v = v_sorted[pl.ds(pl.multiple_of(g * rows, rows), rows), :]
                probs = (strip[i * CHUNK + u] * inverse).astype(jnp.bfloat16)
                acc = acc + lax.dot_general(
                    probs, v, (((1,), (0,)), ((), ())), preferred_element_type=jnp.float32
                )
            return acc

        acc = lax.fori_loop(0, chunks, weigh, jnp.zeros((rows, dim), jnp.float32))
        rounded = acc.astype(jnp.bfloat16)
        attn_out[at_q, :] = rounded
        wide = rounded.astype(jnp.float32)
        square_out[pl.ds(c, 1), :] = gate[pl.ds(c, 1), :] * jnp.sum(wide * wide, axis=0, keepdims=True)
        return carry

    lax.fori_loop(0, groups, one_group, 0)


def attend(place, start, qkv, gate, per_group, groups):
    block_len, dim = qkv.shape[1], qkv.shape[2]
    length = per_group * groups * block_len
    rows = per_group * block_len
    smem = pl.BlockSpec(memory_space=pltpu.SMEM)
    vmem = pl.BlockSpec(memory_space=pltpu.VMEM)
    padded = length + (CHUNK - 1) * rows
    return pl.pallas_call(
        functools.partial(attend_kernel, per_group=per_group, groups=groups),
        in_specs=[smem, smem, vmem, vmem],
        out_specs=[vmem, vmem],
        out_shape=[
            jax.ShapeDtypeStruct((length, dim), jnp.bfloat16),
            jax.ShapeDtypeStruct((groups, dim), jnp.float32),
        ],
        scratch_shapes=[
            pltpu.VMEM((length, dim), jnp.bfloat16),
            pltpu.VMEM((padded, dim), jnp.bfloat16),
            pltpu.VMEM((padded, dim), jnp.bfloat16),
            pltpu.VMEM((groups + CHUNK, rows, rows), jnp.float32),
        ],
        compiler_params=pltpu.CompilerParams(vmem_limit_bytes=40 * 1024 * 1024),
        cost_estimate=pl.CostEstimate(
            flops=4 * length * length * dim, bytes_accessed=4 * length * dim * 2, transcendentals=length * length
        ),
    )(place, start, qkv, gate)


def combine_kernel(place, attn, square, diff, out, *, per_group, groups):
    block_len, dim = diff.shape[1], diff.shape[2]

    for c in range(groups):
        acc = jnp.zeros((8, dim), jnp.float32)
        for b in range(per_group):
            t = c * per_group + b
            product = attn[t * block_len : (t + 1) * block_len, :].astype(jnp.float32) * diff[
                place[t]
            ].astype(jnp.float32)
            acc = acc + jnp.sum(product.reshape(block_len // 8, 8, dim), axis=0)
        row = jnp.sum(acc, axis=0, keepdims=True) + square[c : c + 1, :]
        for copy in range(out.shape[0]):
            out[copy, c : c + 1, :] = row


def combine(place, attn, square, diff, copies, per_group, groups):
    smem = pl.BlockSpec(memory_space=pltpu.SMEM)
    vmem = pl.BlockSpec(memory_space=pltpu.VMEM)
    return pl.pallas_call(
        functools.partial(combine_kernel, per_group=per_group, groups=groups),
        in_specs=[smem, vmem, vmem, vmem],
        out_specs=vmem,
        out_shape=jax.ShapeDtypeStruct((copies, groups, attn.shape[1]), jnp.float32),
    )(place, attn, square, diff)


def finish_kernel(sums, embed, out, *, root):
    out[...] = (
        lax.dot_general(
            sums[...],
            embed[...],
            (((0,), (0,)), ((), ())),
            precision=lax.Precision.HIGHEST,
            preferred_element_type=jnp.float32,
        )
        / root
    )


def finish(sums, embed, root):
    return pl.pallas_call(
        functools.partial(finish_kernel, root=root),
        out_shape=jax.ShapeDtypeStruct((sums.shape[1], embed.shape[1]), jnp.float32),
    )(sums, embed)


def sinusoid(noise, emb_width):
    half_width = emb_width // 2
    frequency = jnp.exp(-math.log(10000.0) * jnp.arange(half_width, dtype=jnp.float32) / half_width)
    angles = 1000.0 * noise[..., None] * frequency
    return jnp.concatenate([jnp.cos(angles), jnp.sin(angles)], -1).astype(jnp.bfloat16)


def exchange(value, axis):
    return lax.all_to_all(value, axis, split_axis=0, concat_axis=0, tiled=True)


def per_device(
    query, key, value, latent, target, noise_level, mod_weight, block_order, context_start
):
    frames = lax.axis_size("frame")
    streams = lax.axis_size("stream")
    index = lax.axis_index("frame")
    tokens, width = query.shape[1:]
    block_len = tokens // 2
    local_width = width // frames
    blocks = block_order.shape[0]
    groups = noise_level.shape[1]
    per_group = blocks // groups
    root = math.sqrt(per_group * block_len)

    noise_all = exchange(jnp.broadcast_to(noise_level[None], (streams, 1, groups)), "stream")
    embed_all = sinusoid(noise_all.reshape(streams * groups), mod_weight.shape[1])
    embed_own = sinusoid(noise_level[0], mod_weight.shape[1])
    weight_rows = lax.dynamic_slice_in_dim(mod_weight, index * local_width, local_width, 0)
    gate = lax.dot_general(
        embed_own, weight_rows, (((1,), (1,)), ((), ())), preferred_element_type=jnp.float32
    )
    times = jnp.arange(blocks, dtype=jnp.int32)
    place = jnp.sum(jnp.where(block_order[None, :] == times[:, None], times[None, :], 0), axis=1)

    qkv = to_panels(panels_kernel, (query[0], key[0], value[0]), frames, 3)
    diff = to_panels(difference_kernel, (latent[0], target[0]), frames, 1)
    qkv = exchange(qkv, "frame")
    diff = exchange(diff, "frame")
    attn, square = attend(
        place, context_start[0], qkv.reshape(frames * 6, block_len, local_width), gate, per_group, groups
    )
    sums = combine(
        place, attn, square, diff.reshape(frames * 2, block_len, local_width), streams, per_group, groups
    )
    sums = exchange(sums, "stream")
    return finish(
        sums.reshape(streams * groups, local_width), embed_all.astype(jnp.float32), root
    )


def solution(mesh):
    placed = (
        P("stream", "frame", None),
        P("stream", "frame", None),
        P("stream", "frame", None),
        P("stream", "frame", None),
        P("stream", "frame", None),
        P("stream", None),
        P(),
        P(),
        P("stream", None),
    )
    return jax.shard_map(
        per_device, mesh=mesh, in_specs=placed, out_specs=P("frame", None), check_vma=False
    )
```

```python
import functools
import math

import jax
import jax.numpy as jnp
from jax import lax
from jax.experimental import pallas as pl
from jax.experimental.pallas import tpu as pltpu
from jax.sharding import PartitionSpec as P


CHUNK = 4


def panels_kernel(*refs, panel):
    ins, out = refs[:-1], refs[-1]
    rows = ins[0].shape[0]
    for k in range(out.shape[0]):
        for a, ref in enumerate(ins):
            out[k, a * rows : (a + 1) * rows, :] = ref[:, k * panel : (k + 1) * panel]


def difference_kernel(latent, target, out, *, panel):
    for k in range(out.shape[0]):
        part = slice(k * panel, (k + 1) * panel)
        wide = latent[:, part].astype(jnp.float32) - target[:, part].astype(jnp.float32)
        out[k] = wide.astype(jnp.bfloat16)


def to_panels(kernel, arrays, frames, stacked):
    rows, width = arrays[0].shape
    panel = width // frames
    step = max(1, frames // 4)
    return pl.pallas_call(
        functools.partial(kernel, panel=panel),
        grid=(frames // step,),
        in_specs=[pl.BlockSpec((rows, step * panel), lambda i: (0, i))] * len(arrays),
        out_specs=pl.BlockSpec((step, stacked * rows, panel), lambda i: (i, 0, 0)),
        out_shape=jax.ShapeDtypeStruct((frames, stacked * rows, panel), jnp.bfloat16),
    )(*arrays)


def attend_kernel(
    place, start, qkv, gate, attn_out, square_out, q_sorted, k_sorted, v_sorted, strip, *, per_group, groups
):
    block_len, dim = qkv.shape[1], qkv.shape[2]
    blocks = per_group * groups
    rows = per_group * block_len
    scale = 1.0 / math.sqrt(dim)

    def sort_block(t, carry):
        p = place[t]
        base = (p // 2) * 6 + p % 2
        at = pl.ds(pl.multiple_of(t * block_len, block_len), block_len)
        q_sorted[at, :] = qkv[base]
        k_sorted[at, :] = qkv[base + 2]
        v_sorted[at, :] = qkv[base + 4]
        return carry

    lax.fori_loop(0, blocks, sort_block, 0, unroll=8)
    pad = jnp.zeros(((CHUNK - 1) * rows, dim), jnp.bfloat16)
    k_sorted[blocks * block_len :, :] = pad
    v_sorted[blocks * block_len :, :] = pad

    def one_group(c, carry):
        first = start[c]
        count = c - first + 1
        chunks = (count + CHUNK - 1) // CHUNK
        at_q = pl.ds(pl.multiple_of(c * rows, rows), rows)
        q = q_sorted[at_q, :]

        def scores(i, peak):
            for u in range(CHUNK):
                g = first + i * CHUNK + u
                k = k_sorted[pl.ds(pl.multiple_of(g * rows, rows), rows), :]
                s = lax.dot_general(
                    q, k, (((1,), (1,)), ((), ())), preferred_element_type=jnp.float32
                )
                s = jnp.where(g <= c, s * scale, -jnp.inf)
                strip[i * CHUNK + u] = s
                for b in range(rows // 128):
                    peak = jnp.maximum(peak, s[:, b * 128 : (b + 1) * 128])
            return peak

        peak = lax.fori_loop(0, chunks, scores, jnp.full((rows, 128), -jnp.inf, jnp.float32))
        peak = jnp.max(peak, axis=1, keepdims=True)

        def exponents(i, total):
            for u in range(CHUNK):
                e = jnp.exp(strip[i * CHUNK + u] - peak)
                strip[i * CHUNK + u] = e
                for b in range(rows // 128):
                    total = total + e[:, b * 128 : (b + 1) * 128]
            return total

        total = lax.fori_loop(0, chunks, exponents, jnp.zeros((rows, 128), jnp.float32))
        inverse = 1.0 / jnp.sum(total, axis=1, keepdims=True)

        def weigh(i, acc):
            for u in range(CHUNK):
                g = first + i * CHUNK + u
                v = v_sorted[pl.ds(pl.multiple_of(g * rows, rows), rows), :]
                probs = (strip[i * CHUNK + u] * inverse).astype(jnp.bfloat16)
                acc = acc + lax.dot_general(
                    probs, v, (((1,), (0,)), ((), ())), preferred_element_type=jnp.float32
                )
            return acc

        acc = lax.fori_loop(0, chunks, weigh, jnp.zeros((rows, dim), jnp.float32))
        rounded = acc.astype(jnp.bfloat16)
        attn_out[at_q, :] = rounded
        wide = rounded.astype(jnp.float32)
        square_out[pl.ds(c, 1), :] = gate[pl.ds(c, 1), :] * jnp.sum(wide * wide, axis=0, keepdims=True)
        return carry

    lax.fori_loop(0, groups, one_group, 0)


def attend(place, start, qkv, gate, per_group, groups):
    block_len, dim = qkv.shape[1], qkv.shape[2]
    length = per_group * groups * block_len
    rows = per_group * block_len
    smem = pl.BlockSpec(memory_space=pltpu.SMEM)
    vmem = pl.BlockSpec(memory_space=pltpu.VMEM)
    padded = length + (CHUNK - 1) * rows
    return pl.pallas_call(
        functools.partial(attend_kernel, per_group=per_group, groups=groups),
        in_specs=[smem, smem, vmem, vmem],
        out_specs=[vmem, vmem],
        out_shape=[
            jax.ShapeDtypeStruct((length, dim), jnp.bfloat16),
            jax.ShapeDtypeStruct((groups, dim), jnp.float32),
        ],
        scratch_shapes=[
            pltpu.VMEM((length, dim), jnp.bfloat16),
            pltpu.VMEM((padded, dim), jnp.bfloat16),
            pltpu.VMEM((padded, dim), jnp.bfloat16),
            pltpu.VMEM((groups + CHUNK, rows, rows), jnp.float32),
        ],
        compiler_params=pltpu.CompilerParams(vmem_limit_bytes=40 * 1024 * 1024),
        cost_estimate=pl.CostEstimate(
            flops=4 * length * length * dim, bytes_accessed=4 * length * dim * 2, transcendentals=length * length
        ),
    )(place, start, qkv, gate)


def combine_kernel(when, attn, square, *refs, per_group):
    parts, out, sums = refs[:-2], refs[-2], refs[-1]
    block_len, _ = parts[0].shape[1:]
    sums[...] = square[...]
    at = 0
    for part in parts:
        for k in range(part.shape[0]):
            t = when[at]
            at += 1
            rows = pl.ds(pl.multiple_of(t * block_len, block_len), block_len)
            product = attn[rows, :].astype(jnp.float32) * part[k].astype(jnp.float32)
            row = pl.ds(t // per_group, 1)
            sums[row, :] = sums[row, :] + jnp.sum(product, axis=0, keepdims=True)
    for copy in range(out.shape[0]):
        out[copy] = sums[...]


def combine(when, attn, square, parts, copies, per_group):
    smem = pl.BlockSpec(memory_space=pltpu.SMEM)
    vmem = pl.BlockSpec(memory_space=pltpu.VMEM)
    return pl.pallas_call(
        functools.partial(combine_kernel, per_group=per_group),
        in_specs=[smem, vmem, vmem] + [vmem] * len(parts),
        out_specs=vmem,
        out_shape=jax.ShapeDtypeStruct((copies, *square.shape), jnp.float32),
        scratch_shapes=[pltpu.VMEM(square.shape, jnp.float32)],
        compiler_params=pltpu.CompilerParams(vmem_limit_bytes=16 * 1024 * 1024),
    )(when, attn, square, *parts)


def finish_kernel(sums, embed, out, *, root):
    out[...] = (
        lax.dot_general(
            sums[...],
            embed[...],
            (((0,), (0,)), ((), ())),
            precision=lax.Precision.HIGHEST,
            preferred_element_type=jnp.float32,
        )
        / root
    )


def finish(sums, embed, root):
    return pl.pallas_call(
        functools.partial(finish_kernel, root=root),
        out_shape=jax.ShapeDtypeStruct((sums.shape[1], embed.shape[1]), jnp.float32),
        compiler_params=pltpu.CompilerParams(vmem_limit_bytes=16 * 1024 * 1024),
    )(sums, embed)


def sinusoid(noise, emb_width):
    half_width = emb_width // 2
    frequency = jnp.exp(-math.log(10000.0) * jnp.arange(half_width, dtype=jnp.float32) / half_width)
    angles = 1000.0 * noise[..., None] * frequency
    return jnp.concatenate([jnp.cos(angles), jnp.sin(angles)], -1).astype(jnp.bfloat16)


def exchange(value, axis):
    return lax.all_to_all(value, axis, split_axis=0, concat_axis=0, tiled=True)


def swap(value, axis, mask):
    pairs = [(i, i ^ mask) for i in range(lax.axis_size(axis))]
    return lax.ppermute(value, axis, pairs)


def exchange_by_swaps(panels, index):
    near = (0, 1, 16, 17)
    shape = panels.shape[1:]
    cube = panels.reshape(2, 8, 2, *shape)
    first = []
    for mask in near:
        sent = lax.dynamic_slice(
            cube,
            ((index >> 4) ^ (mask >> 4), 0, (index & 1) ^ (mask & 1)) + (0,) * len(shape),
            (1, 8, 1, *shape),
        ).reshape(8, *shape)
        first.append(sent if mask == 0 else swap(sent, "frame", mask))
    first = jnp.stack(first, axis=1)
    parts = []
    for z in range(8):
        sent = lax.dynamic_index_in_dim(first, ((index >> 1) & 7) ^ z, 0, keepdims=False)
        parts.append(sent if z == 0 else swap(sent, "frame", 2 * z))
    masks = [m + 2 * z for z in range(8) for m in near]
    return parts, masks


def per_device(
    query, key, value, latent, target, noise_level, mod_weight, block_order, context_start
):
    frames = lax.axis_size("frame")
    streams = lax.axis_size("stream")
    index = lax.axis_index("frame")
    tokens, width = query.shape[1:]
    block_len = tokens // 2
    local_width = width // frames
    blocks = block_order.shape[0]
    groups = noise_level.shape[1]
    per_group = blocks // groups
    root = math.sqrt(per_group * block_len)

    stream = lax.axis_index("stream")
    qkv = to_panels(panels_kernel, (query[0], key[0], value[0]), frames, 3)
    qkv = exchange(qkv, "frame")
    diff = to_panels(difference_kernel, (latent[0], target[0]), frames, 1)
    parts, masks = exchange_by_swaps(diff, index)
    noise = noise_level
    for mask in (1, 2, 4):
        noise = jnp.concatenate([noise, swap(noise, "stream", mask)])
    owner = jnp.arange(streams, dtype=jnp.int32) ^ stream
    pick = owner[None, :] == jnp.arange(streams, dtype=jnp.int32)[:, None]
    noise_all = jnp.sum(jnp.where(pick[:, :, None], noise[None], 0.0), axis=1)
    embed_all = sinusoid(noise_all.reshape(streams * groups), mod_weight.shape[1])
    embed_own = sinusoid(noise_level[0], mod_weight.shape[1])
    weight_rows = lax.dynamic_slice_in_dim(mod_weight, index * local_width, local_width, 0)
    gate = lax.dot_general(
        embed_own, weight_rows, (((1,), (1,)), ((), ())), preferred_element_type=jnp.float32
    )
    times = jnp.arange(blocks, dtype=jnp.int32)
    place = jnp.sum(jnp.where(block_order[None, :] == times[:, None], times[None, :], 0), axis=1)
    slots = jnp.array([2 * m + b for m in masks for b in range(2)], jnp.int32) ^ (2 * index)
    when = jnp.sum(jnp.where(slots[:, None] == times[None, :], block_order[None, :], 0), axis=1)
    attn, square = attend(
        place, context_start[0], qkv.reshape(frames * 6, block_len, local_width), gate, per_group, groups
    )
    parts = [p.reshape(-1, block_len, local_width) for p in parts]
    sums = combine(when, attn, square, parts, streams, per_group)
    sums = exchange(sums, "stream")
    return finish(sums.reshape(streams * groups, local_width), embed_all.astype(jnp.float32), root)


def solution(mesh):
    placed = (
        P("stream", "frame", None),
        P("stream", "frame", None),
        P("stream", "frame", None),
        P("stream", "frame", None),
        P("stream", "frame", None),
        P("stream", None),
        P(),
        P(),
        P("stream", None),
    )
    return jax.shard_map(
        per_device, mesh=mesh, in_specs=placed, out_specs=P("frame", None), check_vma=False
    )
```

```python
import functools
import math

import jax
import jax.numpy as jnp
from jax import lax
from jax.experimental import pallas as pl
from jax.experimental.pallas import tpu as pltpu
from jax.sharding import PartitionSpec as P


CHUNK = 4
ROWS = 32


def panels_kernel(*refs, panel):
    ins, out = refs[:-1], refs[-1]
    rows = ins[0].shape[0]
    for k in range(out.shape[0]):
        for a, ref in enumerate(ins):
            out[k, a * rows : (a + 1) * rows, :] = ref[:, k * panel : (k + 1) * panel]


def difference_kernel(latent, target, out, *, panel):
    for k in range(out.shape[0]):
        part = slice(k * panel, (k + 1) * panel)
        wide = latent[:, part].astype(jnp.float32) - target[:, part].astype(jnp.float32)
        out[k] = wide.astype(jnp.bfloat16)


def to_panels(kernel, arrays, frames, stacked, limit=None, steps=2):
    rows, width = arrays[0].shape
    panel = width // frames
    step = max(1, frames // steps)
    return pl.pallas_call(
        functools.partial(kernel, panel=panel),
        grid=(frames // step,),
        in_specs=[pl.BlockSpec((rows, step * panel), lambda i: (0, i))] * len(arrays),
        out_specs=pl.BlockSpec((step, stacked * rows, panel), lambda i: (i, 0, 0)),
        out_shape=jax.ShapeDtypeStruct((frames, stacked * rows, panel), jnp.bfloat16),
        compiler_params=pltpu.CompilerParams(vmem_limit_bytes=limit),
    )(*arrays)


def attend_kernel(
    order,
    start,
    qkv,
    gate,
    attn_out,
    square_out,
    landing,
    q_sorted,
    k_sorted,
    v_sorted,
    strip,
    levels,
    tops,
    totals,
    group_of,
    tile_of,
    sems,
    *,
    per_group,
    groups,
):
    block_len, dim = qkv.shape[1], qkv.shape[2]
    blocks = per_group * groups
    rows = per_group * block_len
    wide = CHUNK * rows
    factor = math.log2(math.e) / math.sqrt(dim)
    pieces = sems.shape[0]
    piece = qkv.shape[0] // pieces

    def fetch(n):
        part = pl.ds(n * piece, piece)
        return pltpu.make_async_copy(qkv.at[part], landing.at[part], sems.at[n])

    for n in range(pieces):
        fetch(n).start()

    def list_group(c, at):
        def list_chunk(j, at):
            group_of[at] = c
            tile_of[at] = start[c] + j * CHUNK
            return at + 1

        return lax.fori_loop(0, (c - start[c] + CHUNK) // CHUNK, list_chunk, at)

    chunks = lax.fori_loop(0, groups, list_group, 0)

    pad = jnp.zeros(((CHUNK - 1) * rows, dim), jnp.bfloat16)
    k_sorted[blocks * block_len :, :] = pad
    v_sorted[blocks * block_len :, :] = pad
    levels[...] = jnp.zeros(levels.shape, jnp.float32)
    per_piece = blocks // pieces
    for n in range(pieces):
        fetch(n).wait()

        def sort_block(p, carry):
            base = (p // 2) * 6 + p % 2
            at = pl.ds(pl.multiple_of(order[p] * block_len, block_len), block_len)
            q_sorted[at, :] = landing[base]
            k_sorted[at, :] = landing[base + 2]
            v_sorted[at, :] = landing[base + 4]
            return carry

        lax.fori_loop(n * per_piece, (n + 1) * per_piece, sort_block, 0, unroll=8)

    def rows_of(ref, tile, count):
        return ref[pl.ds(pl.multiple_of(tile * rows, rows), count), :]

    def scores(t):
        c, tile = group_of[t], tile_of[t]
        s = lax.dot_general(
            rows_of(q_sorted, c, rows),
            rows_of(k_sorted, tile, wide),
            (((1,), (1,)), ((), ())),
            preferred_element_type=jnp.float32,
        )
        strip[t] = s

    def normalize(t):
        c, tile = group_of[t], tile_of[t]
        fresh = tile == start[c]
        for r in range(0, rows, ROWS):
            at_r = slice(r, r + ROWS)
            peak = None
            for u in range(CHUNK):
                top = strip[t, at_r, u * rows : u * rows + 128]
                for b in range(1, rows // 128):
                    top = jnp.maximum(top, strip[t, at_r, u * rows + b * 128 : u * rows + (b + 1) * 128])
                peak = top if u == 0 else jnp.maximum(peak, jnp.where(tile + u <= c, top, -jnp.inf))
            peak = jnp.broadcast_to(jnp.max(peak, axis=1, keepdims=True) * factor, (ROWS, 128))
            before = jnp.where(fresh, -jnp.inf, tops[at_r, :])
            top = jnp.maximum(before, peak)
            total = totals[at_r, :] * jnp.exp2(before - top)
            for u in range(CHUNK):
                here = jnp.where(tile + u <= c, top, jnp.inf)
                for b in range(rows // 128):
                    at = u * rows + b * 128
                    total = total + jnp.exp2(strip[t, at_r, at : at + 128] * factor - here)
            tops[at_r, :] = top
            totals[at_r, :] = total
            level = top + jnp.log2(jnp.sum(total, axis=1, keepdims=True))
            lanes = lax.broadcasted_iota(jnp.int32, (ROWS, 128), 1)
            levels[at_r, :] = jnp.where(lanes == c, level, levels[at_r, :])

    def first_pass(t, carry):
        normalize(t - 1)
        scores(t)
        return carry

    totals[...] = jnp.zeros(totals.shape, jnp.float32)
    tops[...] = jnp.zeros(tops.shape, jnp.float32)
    scores(0)
    lax.fori_loop(1, chunks, first_pass, 0)
    normalize(chunks - 1)

    def level_of(c):
        lanes = lax.broadcasted_iota(jnp.int32, levels.shape, 1)
        level = jnp.sum(jnp.where(lanes == c, levels[...], 0.0), axis=1, keepdims=True)
        return jnp.broadcast_to(level, (rows, 128))

    def second_pass(t, carry):
        acc, level = carry
        c, tile = group_of[t], tile_of[t]
        probs = []
        for u in range(CHUNK):
            here = jnp.where(tile + u <= c, level, jnp.inf)
            for b in range(rows // 128):
                at = u * rows + b * 128
                probs.append(jnp.exp2(strip[t, :, at : at + 128] * factor - here).astype(jnp.bfloat16))
        part = lax.dot_general(
            jnp.concatenate(probs, axis=1),
            rows_of(v_sorted, tile, wide),
            (((1,), (0,)), ((), ())),
            preferred_element_type=jnp.float32,
        )
        level = level_of(group_of[jnp.minimum(t + 1, chunks - 1)])
        acc = jnp.where(tile == start[c], 0.0, acc) + part
        rounded = acc.astype(jnp.bfloat16)
        attn_out[pl.ds(pl.multiple_of(c * rows, rows), rows), :] = rounded
        back = rounded.astype(jnp.float32)
        square_out[pl.ds(c, 1), :] = gate[pl.ds(c, 1), :] * jnp.sum(back * back, axis=0, keepdims=True)
        return acc, level

    lax.fori_loop(0, chunks, second_pass, (jnp.zeros((rows, dim), jnp.float32), level_of(0)))


def attend(order, start, qkv, gate, per_group, groups):
    block_len, dim = qkv.shape[1], qkv.shape[2]
    length = per_group * groups * block_len
    rows = per_group * block_len
    smem = pl.BlockSpec(memory_space=pltpu.SMEM)
    vmem = pl.BlockSpec(memory_space=pltpu.VMEM)
    padded = length + (CHUNK - 1) * rows
    most = sum((c + CHUNK) // CHUNK for c in range(groups))
    return pl.pallas_call(
        functools.partial(attend_kernel, per_group=per_group, groups=groups),
        in_specs=[smem, smem, pl.BlockSpec(memory_space=pl.ANY), vmem],
        out_specs=[vmem, vmem],
        out_shape=[
            jax.ShapeDtypeStruct((length, dim), jnp.bfloat16),
            jax.ShapeDtypeStruct((groups, dim), jnp.float32),
        ],
        scratch_shapes=[
            pltpu.VMEM(qkv.shape, jnp.bfloat16),
            pltpu.VMEM((length, dim), jnp.bfloat16),
            pltpu.VMEM((padded, dim), jnp.bfloat16),
            pltpu.VMEM((padded, dim), jnp.bfloat16),
            pltpu.VMEM((most, rows, CHUNK * rows), jnp.float32),
            pltpu.VMEM((rows, 128), jnp.float32),
            pltpu.VMEM((rows, 128), jnp.float32),
            pltpu.VMEM((rows, 128), jnp.float32),
            pltpu.SMEM((most,), jnp.int32),
            pltpu.SMEM((most,), jnp.int32),
            pltpu.SemaphoreType.DMA((4,)),
        ],
        compiler_params=pltpu.CompilerParams(vmem_limit_bytes=50 * 1024 * 1024),
    )(order, start, qkv, gate)


def combine_kernel(when, attn, square, *refs, per_group):
    parts, out, sums = refs[:-2], refs[-2], refs[-1]
    block_len, dim = parts[0].shape[1:]
    at = 0
    for part in parts:
        for k in range(part.shape[0]):
            t = when[at]
            at += 1
            rows = pl.ds(pl.multiple_of(t * block_len, block_len), block_len)
            product = attn[rows, :].astype(jnp.float32) * part[k].astype(jnp.float32)
            sums[pl.ds(t, 1), :] = jnp.sum(product, axis=0, keepdims=True)
    groups = square.shape[0]
    total = square[...] + jnp.sum(sums[...].reshape(groups, per_group, dim), axis=1)
    for copy in range(out.shape[0]):
        out[copy] = total


def combine(when, attn, square, parts, copies, per_group):
    smem = pl.BlockSpec(memory_space=pltpu.SMEM)
    vmem = pl.BlockSpec(memory_space=pltpu.VMEM)
    return pl.pallas_call(
        functools.partial(combine_kernel, per_group=per_group),
        in_specs=[smem, vmem, vmem] + [vmem] * len(parts),
        out_specs=vmem,
        out_shape=jax.ShapeDtypeStruct((copies, *square.shape), jnp.float32),
        scratch_shapes=[pltpu.VMEM((square.shape[0] * per_group, square.shape[1]), jnp.float32)],
        compiler_params=pltpu.CompilerParams(vmem_limit_bytes=16 * 1024 * 1024),
    )(when, attn, square, *parts)


def finish_kernel(sums, embed, out, *, root):
    out[...] = (
        lax.dot_general(
            sums[...],
            embed[...],
            (((0,), (0,)), ((), ())),
            precision=lax.Precision.HIGHEST,
            preferred_element_type=jnp.float32,
        )
        / root
    )


def finish(sums, embed, root):
    return pl.pallas_call(
        functools.partial(finish_kernel, root=root),
        out_shape=jax.ShapeDtypeStruct((sums.shape[1], embed.shape[1]), jnp.float32),
        compiler_params=pltpu.CompilerParams(vmem_limit_bytes=16 * 1024 * 1024),
    )(sums, embed)


def sinusoid(noise, emb_width):
    half_width = emb_width // 2
    frequency = jnp.exp(-math.log(10000.0) * jnp.arange(half_width, dtype=jnp.float32) / half_width)
    angles = 1000.0 * noise[..., None] * frequency
    return jnp.concatenate([jnp.cos(angles), jnp.sin(angles)], -1).astype(jnp.bfloat16)


def exchange(value, axis):
    return lax.all_to_all(value, axis, split_axis=0, concat_axis=0, tiled=True)


def swap(value, axis, mask):
    pairs = [(i, i ^ mask) for i in range(lax.axis_size(axis))]
    return lax.ppermute(value, axis, pairs)


def exchange_by_swaps(panels, index):
    near = (0, 1, 16, 17)
    shape = panels.shape[1:]
    cube = panels.reshape(2, 8, 2, *shape)
    first = []
    for mask in near:
        sent = lax.dynamic_slice(
            cube,
            ((index >> 4) ^ (mask >> 4), 0, (index & 1) ^ (mask & 1)) + (0,) * len(shape),
            (1, 8, 1, *shape),
        ).reshape(8, *shape)
        first.append(sent if mask == 0 else swap(sent, "frame", mask))
    first = jnp.stack(first, axis=1)
    parts = []
    for z in range(8):
        sent = lax.dynamic_index_in_dim(first, ((index >> 1) & 7) ^ z, 0, keepdims=False)
        parts.append(sent if z == 0 else swap(sent, "frame", 2 * z))
    masks = [m + 2 * z for z in range(8) for m in near]
    return parts, masks


def per_device(
    query, key, value, latent, target, noise_level, mod_weight, block_order, context_start
):
    frames = lax.axis_size("frame")
    streams = lax.axis_size("stream")
    index = lax.axis_index("frame")
    tokens, width = query.shape[1:]
    block_len = tokens // 2
    local_width = width // frames
    blocks = block_order.shape[0]
    groups = noise_level.shape[1]
    per_group = blocks // groups
    root = math.sqrt(per_group * block_len)

    stream = lax.axis_index("stream")
    qkv = to_panels(panels_kernel, (query[0], key[0], value[0]), frames, 3)
    qkv = exchange(qkv, "frame")
    diff = to_panels(difference_kernel, (latent[0], target[0]), frames, 1, 16 * 1024 * 1024)
    parts, masks = exchange_by_swaps(diff, index)
    noise = noise_level
    for mask in (1, 2, 4):
        noise = jnp.concatenate([noise, swap(noise, "stream", mask)])
    owner = jnp.arange(streams, dtype=jnp.int32) ^ stream
    pick = owner[None, :] == jnp.arange(streams, dtype=jnp.int32)[:, None]
    noise_all = jnp.sum(jnp.where(pick[:, :, None], noise[None], 0.0), axis=1)
    embed_all = sinusoid(noise_all.reshape(streams * groups), mod_weight.shape[1])
    embed_own = sinusoid(noise_level[0], mod_weight.shape[1])
    weight_rows = lax.dynamic_slice_in_dim(mod_weight, index * local_width, local_width, 0)
    gate = lax.dot_general(
        embed_own, weight_rows, (((1,), (1,)), ((), ())), preferred_element_type=jnp.float32
    )
    times = jnp.arange(blocks, dtype=jnp.int32)
    slots = jnp.array([2 * m + b for m in masks for b in range(2)], jnp.int32) ^ (2 * index)
    when = jnp.sum(jnp.where(slots[:, None] == times[None, :], block_order[None, :], 0), axis=1)
    attn, square = attend(
        block_order, context_start[0], qkv.reshape(frames * 6, block_len, local_width), gate, per_group, groups
    )
    parts = [p.reshape(-1, block_len, local_width) for p in parts]
    sums = combine(when, attn, square, parts, streams, per_group)
    sums = exchange(sums, "stream")
    return finish(sums.reshape(streams * groups, local_width), embed_all.astype(jnp.float32), root)


def solution(mesh):
    placed = (
        P("stream", "frame", None),
        P("stream", "frame", None),
        P("stream", "frame", None),
        P("stream", "frame", None),
        P("stream", "frame", None),
        P("stream", None),
        P(),
        P(),
        P("stream", None),
    )
    return jax.shard_map(
        per_device, mesh=mesh, in_specs=placed, out_specs=P("frame", None), check_vma=False
    )
```

```python
import functools
import math

import jax
import jax.numpy as jnp
from jax import lax
from jax.experimental import pallas as pl
from jax.experimental.pallas import tpu as pltpu
from jax.sharding import PartitionSpec as P


CHUNK = 3
LIMIT = 52 * 1024 * 1024
ROWS = 32


def panels_kernel(*refs, panel):
    ins, out = refs[:-1], refs[-1]
    rows = ins[0].shape[0]
    for k in range(out.shape[0]):
        for a, ref in enumerate(ins):
            out[k, a * rows : (a + 1) * rows, :] = ref[:, k * panel : (k + 1) * panel]


def difference_kernel(latent, target, out, *, panel):
    for k in range(out.shape[0]):
        part = slice(k * panel, (k + 1) * panel)
        wide = latent[:, part].astype(jnp.float32) - target[:, part].astype(jnp.float32)
        out[k] = wide.astype(jnp.bfloat16)


def to_panels(kernel, arrays, frames, stacked, limit=None, steps=2):
    rows, width = arrays[0].shape
    panel = width // frames
    step = max(1, frames // steps)
    return pl.pallas_call(
        functools.partial(kernel, panel=panel),
        grid=(frames // step,),
        in_specs=[pl.BlockSpec((rows, step * panel), lambda i: (0, i))] * len(arrays),
        out_specs=pl.BlockSpec((step, stacked * rows, panel), lambda i: (i, 0, 0)),
        out_shape=jax.ShapeDtypeStruct((frames, stacked * rows, panel), jnp.bfloat16),
        compiler_params=pltpu.CompilerParams(vmem_limit_bytes=limit),
    )(*arrays)


def attend_kernel(
    order,
    start,
    qkv,
    gate,
    attn_out,
    square_out,
    landing,
    q_sorted,
    k_sorted,
    v_sorted,
    even,
    odd,
    levels,
    tops,
    totals,
    group_of,
    tile_of,
    sems,
    *,
    per_group,
    groups,
):
    block_len, dim = qkv.shape[1], qkv.shape[2]
    blocks = per_group * groups
    rows = per_group * block_len
    wide = CHUNK * rows
    factor = math.log2(math.e) / math.sqrt(dim)
    pieces = sems.shape[0]
    piece = qkv.shape[0] // pieces

    def fetch(n):
        part = pl.ds(n * piece, piece)
        return pltpu.make_async_copy(qkv.at[part], landing.at[part], sems.at[n])

    for n in range(pieces):
        fetch(n).start()

    def list_group(c, at):
        def list_chunk(j, at):
            group_of[at] = c
            tile_of[at] = start[c] + j * CHUNK
            return at + 1

        return lax.fori_loop(0, (c - start[c] + CHUNK) // CHUNK, list_chunk, at)

    chunks = lax.fori_loop(0, groups, list_group, 0)
    filler = jnp.minimum(chunks, group_of.shape[0] - 1)
    steps = (chunks + 1) // 2

    @pl.when(chunks % 2 == 1)
    def _():
        group_of[filler] = groups - 1
        tile_of[filler] = groups


    pad = jnp.zeros(((CHUNK - 1) * rows, dim), jnp.bfloat16)
    k_sorted[blocks * block_len :, :] = pad
    v_sorted[blocks * block_len :, :] = pad
    levels[...] = jnp.zeros(levels.shape, jnp.float32)
    per_piece = blocks // pieces
    for n in range(pieces):
        fetch(n).wait()

        def sort_block(p, carry):
            base = (p // 2) * 6 + p % 2
            at = pl.ds(pl.multiple_of(order[p] * block_len, block_len), block_len)
            q_sorted[at, :] = landing[base]
            k_sorted[at, :] = landing[base + 2]
            v_sorted[at, :] = landing[base + 4]
            return carry

        lax.fori_loop(n * per_piece, (n + 1) * per_piece, sort_block, 0, unroll=8)

    def rows_of(ref, tile, count):
        tile = jnp.minimum(tile, groups - 1)
        return ref[pl.ds(pl.multiple_of(tile * rows, rows), count), :]

    def scores(t, strip, slot):
        t = jnp.minimum(t, 2 * steps - 1)
        c, tile = group_of[t], tile_of[t]
        s = lax.dot_general(
            rows_of(q_sorted, c, rows),
            rows_of(k_sorted, tile, wide),
            (((1,), (1,)), ((), ())),
            preferred_element_type=jnp.float32,
        )
        strip[slot] = s

    def normalize(t, strip, slot):
        c, tile = group_of[t], tile_of[t]
        fresh = tile == start[c]
        for r in range(0, rows, ROWS):
            at_r = slice(r, r + ROWS)
            peak = jnp.full((ROWS, 128), -jnp.inf, jnp.float32)
            for u in range(CHUNK):
                top = strip[slot, at_r, u * rows : u * rows + 128]
                for b in range(1, rows // 128):
                    top = jnp.maximum(top, strip[slot, at_r, u * rows + b * 128 : u * rows + (b + 1) * 128])
                peak = jnp.maximum(peak, jnp.where(tile + u <= c, top, -jnp.inf))
            peak = jnp.broadcast_to(jnp.max(peak, axis=1, keepdims=True) * factor, (ROWS, 128))
            before = jnp.where(fresh, -jnp.inf, tops[at_r, :])
            top = jnp.maximum(before, peak)
            total = totals[at_r, :] * jnp.exp2(before - top)
            for u in range(CHUNK):
                here = jnp.where(tile + u <= c, top, jnp.inf)
                for b in range(rows // 128):
                    at = u * rows + b * 128
                    total = total + jnp.exp2(strip[slot, at_r, at : at + 128] * factor - here)
            tops[at_r, :] = top
            totals[at_r, :] = total
            level = top + jnp.log2(jnp.sum(total, axis=1, keepdims=True))
            lanes = lax.broadcasted_iota(jnp.int32, (ROWS, 128), 1)
            levels[at_r, :] = jnp.where(lanes == c, level, levels[at_r, :])

    def first_pass(i, carry):
        normalize(2 * i, even, i)
        scores(2 * i + 1, odd, i)
        normalize(2 * i + 1, odd, i)
        scores(2 * i + 2, even, i + 1)
        return carry

    totals[...] = jnp.zeros(totals.shape, jnp.float32)
    tops[...] = jnp.zeros(tops.shape, jnp.float32)
    scores(0, even, 0)
    lax.fori_loop(0, steps, first_pass, 0)

    def level_of(c):
        lanes = lax.broadcasted_iota(jnp.int32, levels.shape, 1)
        level = jnp.sum(jnp.where(lanes == c, levels[...], 0.0), axis=1, keepdims=True)
        return jnp.broadcast_to(level, (rows, 128))

    def weigh(t, strip, slot, carry):
        acc, level = carry
        c, tile = group_of[t], tile_of[t]
        probs = []
        for u in range(CHUNK):
            here = jnp.where(tile + u <= c, level, jnp.inf)
            for b in range(rows // 128):
                at = u * rows + b * 128
                probs.append(jnp.exp2(strip[slot, :, at : at + 128] * factor - here).astype(jnp.bfloat16))
        part = lax.dot_general(
            jnp.concatenate(probs, axis=1),
            rows_of(v_sorted, tile, wide),
            (((1,), (0,)), ((), ())),
            preferred_element_type=jnp.float32,
        )
        level = level_of(group_of[jnp.minimum(t + 1, 2 * steps - 1)])
        acc = jnp.where(tile == start[c], 0.0, acc) + part
        rounded = acc.astype(jnp.bfloat16)
        attn_out[pl.ds(pl.multiple_of(c * rows, rows), rows), :] = rounded
        back = rounded.astype(jnp.float32)
        square_out[pl.ds(c, 1), :] = gate[pl.ds(c, 1), :] * jnp.sum(back * back, axis=0, keepdims=True)
        return acc, level

    def second_pass(i, carry):
        return weigh(2 * i + 1, odd, i, weigh(2 * i, even, i, carry))

    lax.fori_loop(0, steps, second_pass, (jnp.zeros((rows, dim), jnp.float32), level_of(0)))


def attend(order, start, qkv, gate, per_group, groups):
    block_len, dim = qkv.shape[1], qkv.shape[2]
    length = per_group * groups * block_len
    rows = per_group * block_len
    smem = pl.BlockSpec(memory_space=pltpu.SMEM)
    vmem = pl.BlockSpec(memory_space=pltpu.VMEM)
    padded = length + (CHUNK - 1) * rows
    most = sum((c + CHUNK) // CHUNK for c in range(groups))
    most += most % 2
    return pl.pallas_call(
        functools.partial(attend_kernel, per_group=per_group, groups=groups),
        in_specs=[smem, smem, pl.BlockSpec(memory_space=pl.ANY), vmem],
        out_specs=[vmem, vmem],
        out_shape=[
            jax.ShapeDtypeStruct((length, dim), jnp.bfloat16),
            jax.ShapeDtypeStruct((groups, dim), jnp.float32),
        ],
        scratch_shapes=[
            pltpu.VMEM(qkv.shape, jnp.bfloat16),
            pltpu.VMEM((length, dim), jnp.bfloat16),
            pltpu.VMEM((padded, dim), jnp.bfloat16),
            pltpu.VMEM((padded, dim), jnp.bfloat16),
            pltpu.VMEM((most // 2 + 1, rows, CHUNK * rows), jnp.float32),
            pltpu.VMEM((most // 2, rows, CHUNK * rows), jnp.float32),
            pltpu.VMEM((rows, 128), jnp.float32),
            pltpu.VMEM((rows, 128), jnp.float32),
            pltpu.VMEM((rows, 128), jnp.float32),
            pltpu.SMEM((most,), jnp.int32),
            pltpu.SMEM((most,), jnp.int32),
            pltpu.SemaphoreType.DMA((4,)),
        ],
        compiler_params=pltpu.CompilerParams(vmem_limit_bytes=LIMIT),
    )(order, start, qkv, gate)


def combine_kernel(when, attn, square, *refs, per_group):
    parts, out, sums = refs[:-2], refs[-2], refs[-1]
    block_len, dim = parts[0].shape[1:]
    at = 0
    for part in parts:
        for k in range(part.shape[0]):
            t = when[at]
            at += 1
            rows = pl.ds(pl.multiple_of(t * block_len, block_len), block_len)
            product = attn[rows, :].astype(jnp.float32) * part[k].astype(jnp.float32)
            sums[pl.ds(t, 1), :] = jnp.sum(product, axis=0, keepdims=True)
    groups = square.shape[0]
    total = square[...] + jnp.sum(sums[...].reshape(groups, per_group, dim), axis=1)
    for copy in range(out.shape[0]):
        out[copy] = total


def combine(when, attn, square, parts, copies, per_group):
    smem = pl.BlockSpec(memory_space=pltpu.SMEM)
    vmem = pl.BlockSpec(memory_space=pltpu.VMEM)
    return pl.pallas_call(
        functools.partial(combine_kernel, per_group=per_group),
        in_specs=[smem, vmem, vmem] + [vmem] * len(parts),
        out_specs=vmem,
        out_shape=jax.ShapeDtypeStruct((copies, *square.shape), jnp.float32),
        scratch_shapes=[pltpu.VMEM((square.shape[0] * per_group, square.shape[1]), jnp.float32)],
        compiler_params=pltpu.CompilerParams(vmem_limit_bytes=16 * 1024 * 1024),
    )(when, attn, square, *parts)


def finish_kernel(sums, embed, out, *, root):
    out[...] = (
        lax.dot_general(
            sums[...],
            embed[...],
            (((0,), (0,)), ((), ())),
            precision=lax.Precision.HIGHEST,
            preferred_element_type=jnp.float32,
        )
        / root
    )


def finish(sums, embed, root):
    return pl.pallas_call(
        functools.partial(finish_kernel, root=root),
        out_shape=jax.ShapeDtypeStruct((sums.shape[1], embed.shape[1]), jnp.float32),
        compiler_params=pltpu.CompilerParams(vmem_limit_bytes=16 * 1024 * 1024),
    )(sums, embed)


def sinusoid(noise, emb_width):
    half_width = emb_width // 2
    frequency = jnp.exp(-math.log(10000.0) * jnp.arange(half_width, dtype=jnp.float32) / half_width)
    angles = 1000.0 * noise[..., None] * frequency
    return jnp.concatenate([jnp.cos(angles), jnp.sin(angles)], -1).astype(jnp.bfloat16)


def exchange(value, axis):
    return lax.all_to_all(value, axis, split_axis=0, concat_axis=0, tiled=True)


def swap(value, axis, mask):
    pairs = [(i, i ^ mask) for i in range(lax.axis_size(axis))]
    return lax.ppermute(value, axis, pairs)


def exchange_by_swaps(panels, index):
    near = (0, 1, 16, 17)
    shape = panels.shape[1:]
    cube = panels.reshape(2, 8, 2, *shape)
    first = []
    for mask in near:
        sent = lax.dynamic_slice(
            cube,
            ((index >> 4) ^ (mask >> 4), 0, (index & 1) ^ (mask & 1)) + (0,) * len(shape),
            (1, 8, 1, *shape),
        ).reshape(8, *shape)
        first.append(sent if mask == 0 else swap(sent, "frame", mask))
    first = jnp.stack(first, axis=1)
    parts = []
    for z in range(8):
        sent = lax.dynamic_index_in_dim(first, ((index >> 1) & 7) ^ z, 0, keepdims=False)
        parts.append(sent if z == 0 else swap(sent, "frame", 2 * z))
    masks = [m + 2 * z for z in range(8) for m in near]
    return parts, masks


def per_device(
    query, key, value, latent, target, noise_level, mod_weight, block_order, context_start
):
    frames = lax.axis_size("frame")
    streams = lax.axis_size("stream")
    index = lax.axis_index("frame")
    tokens, width = query.shape[1:]
    block_len = tokens // 2
    local_width = width // frames
    blocks = block_order.shape[0]
    groups = noise_level.shape[1]
    per_group = blocks // groups
    root = math.sqrt(per_group * block_len)

    stream = lax.axis_index("stream")
    qkv = to_panels(panels_kernel, (query[0], key[0], value[0]), frames, 3)
    qkv = exchange(qkv, "frame")
    diff = to_panels(difference_kernel, (latent[0], target[0]), frames, 1, 16 * 1024 * 1024)
    parts, masks = exchange_by_swaps(diff, index)
    noise = noise_level
    for mask in (1, 2, 4):
        noise = jnp.concatenate([noise, swap(noise, "stream", mask)])
    owner = jnp.arange(streams, dtype=jnp.int32) ^ stream
    pick = owner[None, :] == jnp.arange(streams, dtype=jnp.int32)[:, None]
    noise_all = jnp.sum(jnp.where(pick[:, :, None], noise[None], 0.0), axis=1)
    embed_all = sinusoid(noise_all.reshape(streams * groups), mod_weight.shape[1])
    embed_own = sinusoid(noise_level[0], mod_weight.shape[1])
    weight_rows = lax.dynamic_slice_in_dim(mod_weight, index * local_width, local_width, 0)
    gate = lax.dot_general(
        embed_own, weight_rows, (((1,), (1,)), ((), ())), preferred_element_type=jnp.float32
    )
    times = jnp.arange(blocks, dtype=jnp.int32)
    slots = jnp.array([2 * m + b for m in masks for b in range(2)], jnp.int32) ^ (2 * index)
    when = jnp.sum(jnp.where(slots[:, None] == times[None, :], block_order[None, :], 0), axis=1)
    attn, square = attend(
        block_order, context_start[0], qkv.reshape(frames * 6, block_len, local_width), gate, per_group, groups
    )
    parts = [p.reshape(-1, block_len, local_width) for p in parts]
    sums = combine(when, attn, square, parts, streams, per_group)
    sums = exchange(sums, "stream")
    return finish(sums.reshape(streams * groups, local_width), embed_all.astype(jnp.float32), root)


def solution(mesh):
    placed = (
        P("stream", "frame", None),
        P("stream", "frame", None),
        P("stream", "frame", None),
        P("stream", "frame", None),
        P("stream", "frame", None),
        P("stream", None),
        P(),
        P(),
        P("stream", None),
    )
    return jax.shard_map(
        per_device, mesh=mesh, in_specs=placed, out_specs=P("frame", None), check_vma=False
    )
```
